32 devices in a mesh: prompts: 2 (over x), model: 4 (over z), resp: 4 (over y, core).
Axes of the slice: x: 2, y: 2, z: 4, core: 2. Of those that a mesh axis runs over, the one named last changes fastest.
Arguments:
- x_prompt: bfloat16 [2048, 3072], P(('prompts', 'resp')), parts along dimension 0
- x_resp: bfloat16 [8, 1024, 3072], P(('prompts', 'resp')), parts along dimension 0
- targets: int32 [8, 1024], P(('prompts', 'resp')), parts along dimension 0
- attn_norm: float32 [2, 3072], replicated
- mlp_norm: float32 [2, 3072], replicated
- w_q: bfloat16 [2, 3072, 24, 128], P(None, None, 'model')
- w_k: bfloat16 [2, 3072, 8, 128], P(None, None, 'model')
- w_v: bfloat16 [2, 3072, 8, 128], P(None, None, 'model')
- w_o: bfloat16 [2, 24, 128, 3072], P(None, 'model')
- w_gate: bfloat16 [2, 3072, 8192], P(None, None, 'model')
- w_up: bfloat16 [2, 3072, 8192], P(None, None, 'model')
- w_down: bfloat16 [2, 8192, 3072], P(None, 'model')
- final_norm: float32 [3072], replicated
- w_head: bfloat16 [3072, 65536], P(None, 'model')
Outputs:
- output: float32 [8, 1024], P(('prompts', 'resp')), parts along dimension 0
There are 2 independent parts. The reference program is written for one: setup_inputs(seed, part) draws one part's arguments, and reference() takes and returns one part's arrays. A program takes and returns all parts, laid end to end along the dimension named above; an argument that names none is the same for every part.
All inputs are finite; a program needn't handle non-finite values.
Results may differ from the reference program's by a relative error of at most 0.00256076.
Values are sent between devices in bfloat16 or wider.
A program may use at most 1 GiB of HBM per device.

```python
import math
import jax
import jax.numpy as jnp
from jax import lax

D_MODEL = 3072
N_HEADS = 24
KV_HEADS = 8
HEAD_DIM = 128
FF_DIM = 8192
PROMPT_DEV = 256
RESP_LEN = 1024
VOCAB_SLICE = 65536
GROUP_SIZE = 4
N_LAYERS = 2
ROPE_BASE = 10000
PROMPT_LEN = PROMPT_DEV * GROUP_SIZE
Q_GROUP = N_HEADS // KV_HEADS
RMS_EPS = 1e-6
NEG_BIG = -1e30


def setup_inputs(seed: int = 0, part: int = 0) -> dict:
    root_key = jax.random.key(seed)
    data_root, weight_root = jax.random.split(root_key)
    data_keys = jax.random.split(jax.random.fold_in(data_root, part), 5)
    weight_keys = jax.random.split(weight_root, 12)

    def normal_weight(rng_key, arr_shape, fan_in, w_gain):
        raw_draw = jax.random.normal(rng_key, arr_shape, jnp.float32)
        return (raw_draw * (w_gain / math.sqrt(fan_in))).astype(jnp.bfloat16)

    def norm_gains(rng_key, arr_shape):
        return jax.random.uniform(rng_key, arr_shape, jnp.float32, 0.5, 1.5)

    prompt_mean = jax.random.normal(data_keys[0], (1, D_MODEL), jnp.float32) * 0.7
    piece_shift = jax.random.normal(data_keys[1], (GROUP_SIZE, 1, D_MODEL), jnp.float32) * 0.7
    prompt_noise = jax.random.normal(data_keys[2], (GROUP_SIZE, PROMPT_DEV, D_MODEL), jnp.float32)
    x_prompt = (prompt_noise + piece_shift + prompt_mean).reshape(PROMPT_LEN, D_MODEL).astype(jnp.bfloat16)
    x_resp = jax.random.normal(data_keys[3], (GROUP_SIZE, RESP_LEN, D_MODEL), jnp.float32).astype(jnp.bfloat16)
    flat_ids = jax.random.randint(data_keys[4], (GROUP_SIZE * RESP_LEN,), 0, VOCAB_SLICE, dtype=jnp.int32)
    slot_ids = jnp.arange(GROUP_SIZE * RESP_LEN)
    flat_ids = jnp.where(slot_ids == 0, VOCAB_SLICE - 1, jnp.where(slot_ids == 1, 0, flat_ids))
    targets = flat_ids.reshape(GROUP_SIZE, RESP_LEN).astype(jnp.int32)
    return {
        'x_prompt': x_prompt,
        'x_resp': x_resp,
        'targets': targets,
        'attn_norm': norm_gains(weight_keys[0], (N_LAYERS, D_MODEL)),
        'mlp_norm': norm_gains(weight_keys[1], (N_LAYERS, D_MODEL)),
        'w_q': normal_weight(weight_keys[2], (N_LAYERS, D_MODEL, N_HEADS, HEAD_DIM), D_MODEL, 1.0),
        'w_k': normal_weight(weight_keys[3], (N_LAYERS, D_MODEL, KV_HEADS, HEAD_DIM), D_MODEL, 1.0),
        'w_v': normal_weight(weight_keys[4], (N_LAYERS, D_MODEL, KV_HEADS, HEAD_DIM), D_MODEL, 1.0),
        'w_o': normal_weight(weight_keys[5], (N_LAYERS, N_HEADS, HEAD_DIM, D_MODEL), N_HEADS * HEAD_DIM, 1.0),
        'w_gate': normal_weight(weight_keys[6], (N_LAYERS, D_MODEL, FF_DIM), D_MODEL, 1.0),
        'w_up': normal_weight(weight_keys[7], (N_LAYERS, D_MODEL, FF_DIM), D_MODEL, 1.0),
        'w_down': normal_weight(weight_keys[8], (N_LAYERS, FF_DIM, D_MODEL), FF_DIM, 1.0),
        'final_norm': norm_gains(weight_keys[9], (D_MODEL,)),
        'w_head': normal_weight(weight_keys[10], (D_MODEL, VOCAB_SLICE), D_MODEL, 3.0),
    }


def rms_norm(x_in, norm_gain):
    x_f = x_in.astype(jnp.float32)
    mean_sq = jnp.mean(x_f * x_f, axis=-1, keepdims=True)
    return (x_f * lax.rsqrt(mean_sq + RMS_EPS) * norm_gain).astype(jnp.bfloat16)


def rope_tables(positions):
    inv_freq = jnp.exp(jnp.arange(0, HEAD_DIM, 2, dtype=jnp.float32) * (-math.log(ROPE_BASE) / HEAD_DIM))
    angles = positions.astype(jnp.float32)[:, None] * inv_freq[None, :]
    return jnp.cos(angles), jnp.sin(angles)


def apply_rope(proj_f, cos_tab, sin_tab):
    half_dim = proj_f.shape[-1] // 2
    lo_half = proj_f[..., :half_dim]
    hi_half = proj_f[..., half_dim:]
    cos_b = cos_tab[:, None, :]
    sin_b = sin_tab[:, None, :]
    return jnp.concatenate([lo_half * cos_b - hi_half * sin_b, hi_half * cos_b + lo_half * sin_b], axis=-1)


def project_heads(hidden, w_mat):
    n_out = w_mat.shape[1] * w_mat.shape[2]
    proj_flat = jnp.dot(hidden, w_mat.reshape(D_MODEL, n_out), preferred_element_type=jnp.float32)
    return proj_flat.reshape(hidden.shape[0], w_mat.shape[1], HEAD_DIM)


def attend(queries, key_rows, val_rows, q_pos, k_pos):
    q_len = queries.shape[0]
    q_grp = queries.reshape(q_len, KV_HEADS, Q_GROUP, HEAD_DIM).astype(jnp.float32)
    scores = jnp.einsum('qhre,khe->hrqk', q_grp, key_rows.astype(jnp.float32)) * (1.0 / math.sqrt(HEAD_DIM))
    scores = jnp.where(k_pos[None, :] <= q_pos[:, None], scores, NEG_BIG)
    attn_probs = jax.nn.softmax(scores, axis=-1).astype(jnp.bfloat16).astype(jnp.float32)
    attn_mix = jnp.einsum('hrqk,khe->qhre', attn_probs, val_rows.astype(jnp.float32))
    return attn_mix.reshape(q_len, N_HEADS, HEAD_DIM).astype(jnp.bfloat16)


def finish_layer(x_in, attn_mix, w_out, gain_mlp, w_gate_l, w_up_l, w_down_l):
    attn_proj = jnp.dot(attn_mix.reshape(attn_mix.shape[0], N_HEADS * HEAD_DIM), w_out.reshape(N_HEADS * HEAD_DIM, D_MODEL), preferred_element_type=jnp.float32)
    x_mid = (x_in.astype(jnp.float32) + attn_proj).astype(jnp.bfloat16)
    hidden = rms_norm(x_mid, gain_mlp)
    gate_proj = jnp.dot(hidden, w_gate_l, preferred_element_type=jnp.float32)
    up_proj = jnp.dot(hidden, w_up_l, preferred_element_type=jnp.float32)
    act_vals = (jax.nn.silu(gate_proj) * up_proj).astype(jnp.bfloat16)
    down_proj = jnp.dot(act_vals, w_down_l, preferred_element_type=jnp.float32)
    return (x_mid.astype(jnp.float32) + down_proj).astype(jnp.bfloat16)


def reference(x_prompt, x_resp, targets, attn_norm, mlp_norm, w_q, w_k, w_v, w_o, w_gate, w_up, w_down, final_norm, w_head):
    prompt_pos = jnp.arange(PROMPT_LEN)
    resp_pos = PROMPT_LEN + jnp.arange(RESP_LEN)
    all_pos = jnp.concatenate([prompt_pos, resp_pos])
    p_cos, p_sin = rope_tables(prompt_pos)
    r_cos, r_sin = rope_tables(resp_pos)

    def kv_of(hidden, layer_idx, cos_tab, sin_tab):
        k_rot = apply_rope(project_heads(hidden, w_k[layer_idx]), cos_tab, sin_tab).astype(jnp.bfloat16)
        v_proj = project_heads(hidden, w_v[layer_idx]).astype(jnp.bfloat16)
        return k_rot, v_proj

    hidden_p = rms_norm(x_prompt, attn_norm[0])
    q_prompt = apply_rope(project_heads(hidden_p, w_q[0]), p_cos, p_sin).astype(jnp.bfloat16)
    k_one, v_one = kv_of(hidden_p, 0, p_cos, p_sin)

    def prompt_block(block_in):
        q_block, pos_block = block_in
        return attend(q_block, k_one, v_one, pos_block, prompt_pos)

    mix_prompt = lax.map(prompt_block, (q_prompt.reshape(GROUP_SIZE, PROMPT_DEV, N_HEADS, HEAD_DIM), prompt_pos.reshape(GROUP_SIZE, PROMPT_DEV)))
    x_prompt_one = finish_layer(x_prompt, mix_prompt.reshape(PROMPT_LEN, N_HEADS, HEAD_DIM), w_o[0], mlp_norm[0], w_gate[0], w_up[0], w_down[0])
    k_two, v_two = kv_of(rms_norm(x_prompt_one, attn_norm[1]), 1, p_cos, p_sin)
    prompt_cache = ((k_one, v_one), (k_two, v_two))

    def one_response(resp_in):
        x_cur, tgt_row = resp_in
        for layer_idx in range(N_LAYERS):
            k_cache, v_cache = prompt_cache[layer_idx]
            hidden = rms_norm(x_cur, attn_norm[layer_idx])
            q_resp = apply_rope(project_heads(hidden, w_q[layer_idx]), r_cos, r_sin).astype(jnp.bfloat16)
            k_resp, v_resp = kv_of(hidden, layer_idx, r_cos, r_sin)
            attn_mix = attend(q_resp, jnp.concatenate([k_cache, k_resp]), jnp.concatenate([v_cache, v_resp]), resp_pos, all_pos)
            x_cur = finish_layer(x_cur, attn_mix, w_o[layer_idx], mlp_norm[layer_idx], w_gate[layer_idx], w_up[layer_idx], w_down[layer_idx])
        logits = jnp.dot(rms_norm(x_cur, final_norm), w_head, preferred_element_type=jnp.float32)
        log_norm = jax.nn.logsumexp(logits, axis=-1)
        picked = jnp.sum(jnp.where(jnp.arange(VOCAB_SLICE)[None, :] == tgt_row[:, None], logits, 0.0), axis=-1)
        return picked - log_norm

    return lax.map(one_response, (x_resp, targets))
```

```python
import math
import jax
import jax.numpy as jnp
from jax import lax
from jax.experimental import pallas as pl
from jax.experimental.pallas import tpu as pltpu
from jax.sharding import PartitionSpec as P

RMS_EPS = 1e-6
ROPE_BASE = 10000.0
NEG_BIG = -1e30
SPLITS = (0, 4, 10, 16)


F32 = jnp.float32
BF16 = jnp.bfloat16


def rms_norm(x_in, norm_gain):
    x_f = x_in.astype(F32)
    mean_sq = jnp.mean(x_f * x_f, axis=-1, keepdims=True)
    return (x_f * lax.rsqrt(mean_sq + RMS_EPS) * norm_gain).astype(BF16)


def rope_tables(positions, head_dim):
    inv_freq = jnp.exp(jnp.arange(0, head_dim, 2, dtype=F32) * (-math.log(ROPE_BASE) / head_dim))
    angles = positions.astype(F32)[:, None] * inv_freq[None, :]
    cos_t, sin_t = jnp.cos(angles), jnp.sin(angles)
    return jnp.concatenate([cos_t, cos_t], axis=1), jnp.concatenate([-sin_t, sin_t], axis=1)


def rope_flat(proj_f, cos_tab, sin_tab):
    head_dim = cos_tab.shape[1]
    half_dim = head_dim // 2
    out = []
    for h in range(proj_f.shape[1] // head_dim):
        lo_half = proj_f[:, h * head_dim:h * head_dim + half_dim]
        hi_half = proj_f[:, h * head_dim + half_dim:(h + 1) * head_dim]
        out.append(lo_half * cos_tab[:, :half_dim] - hi_half * sin_tab[:, half_dim:])
        out.append(hi_half * cos_tab[:, half_dim:] + lo_half * sin_tab[:, half_dim:])
    return jnp.concatenate(out, axis=1)


def attn_kernel(n_free, q_ref, cos_ref, sin_ref, k_ref, v_ref, q_pos_ref, k_pos_ref, out_ref):
    head_dim = k_ref.shape[1]
    scale = 1.0 / math.sqrt(head_dim)
    cos_t, sin_t = cos_ref[...], sin_ref[...]
    seen = k_pos_ref[...] <= q_pos_ref[...]
    contract = (((1,), (1,)), ((), ()))
    for h in range(q_ref.shape[1] // head_dim):
        cols = slice(h * head_dim, (h + 1) * head_dim)
        q_f = q_ref[:, cols]
        q_b = (q_f * cos_t + pltpu.roll(q_f, head_dim // 2, 1) * sin_t).astype(BF16)
        s_own = lax.dot_general(q_b, k_ref[n_free:], contract, preferred_element_type=F32) * scale
        s_own = jnp.where(seen, s_own, NEG_BIG)
        top = jnp.max(s_own, axis=1, keepdims=True)
        if n_free:
            s_free = lax.dot_general(q_b, k_ref[:n_free], contract, preferred_element_type=F32) * scale
            top = jnp.maximum(top, jnp.max(s_free, axis=1, keepdims=True))
            e_free = jnp.exp(s_free - top)
        e_own = jnp.exp(s_own - top)
        total = jnp.sum(e_own, axis=1, keepdims=True)
        if n_free:
            total = total + jnp.sum(e_free, axis=1, keepdims=True)
        inv = 1.0 / total
        mix = jnp.dot((e_own * inv).astype(BF16), v_ref[n_free:], preferred_element_type=F32)
        if n_free:
            mix = mix + jnp.dot((e_free * inv).astype(BF16), v_ref[:n_free], preferred_element_type=F32)
        out_ref[:, cols] = mix.astype(BF16)


def attend(q_f, cos_tab, sin_tab, kv_rows, q_pos, k_pos, n_free, head_dim):
    rows, width = q_f.shape
    n_keys = kv_rows.shape[0]
    n_kv = kv_rows.shape[1] // (2 * head_dim)
    grp = width // n_kv
    tile = 128
    return pl.pallas_call(
        lambda *refs: attn_kernel(n_free, *refs),
        grid=(n_kv, rows // tile),
        in_specs=[
            pl.BlockSpec((tile, grp), lambda g, i: (i, g)),
            pl.BlockSpec((tile, head_dim), lambda g, i: (i, 0)),
            pl.BlockSpec((tile, head_dim), lambda g, i: (i, 0)),
            pl.BlockSpec((n_keys, head_dim), lambda g, i: (0, g)),
            pl.BlockSpec((n_keys, head_dim), lambda g, i: (0, n_kv + g)),
            pl.BlockSpec((tile, 1), lambda g, i: (i, 0)),
            pl.BlockSpec((1, n_keys - n_free), lambda g, i: (0, 0)),
        ],
        out_specs=pl.BlockSpec((tile, grp), lambda g, i: (i, g)),
        out_shape=jax.ShapeDtypeStruct((rows, width), BF16),
        cost_estimate=pl.CostEstimate(flops=4 * rows * n_keys * width, bytes_accessed=6 * rows * width + 2 * n_keys * kv_rows.shape[1],
                                      transcendentals=rows * n_keys * (width // head_dim)),
    )(q_f, cos_tab, sin_tab, kv_rows, kv_rows, q_pos[:, None], k_pos[None, :])


def head_kernel(hid_ref, w_ref, tgt_ref, top_ref, sum_ref, pick_ref):
    step = pl.program_id(0)
    lanes = top_ref.shape[1]
    width = w_ref.shape[1]

    @pl.when(step == 0)
    def _():
        top_ref[...] = jnp.full_like(top_ref, NEG_BIG)
        sum_ref[...] = jnp.zeros_like(sum_ref)
        pick_ref[...] = jnp.zeros_like(pick_ref)

    logits = jnp.dot(hid_ref[...], w_ref[...], preferred_element_type=F32)
    cols = [logits[:, i * lanes:(i + 1) * lanes] for i in range(width // lanes)]
    old = top_ref[...]
    top = old
    for col in cols:
        top = jnp.maximum(top, col)
    total = sum_ref[...] * jnp.exp(old - top)
    pick = pick_ref[...]
    lane = lax.broadcasted_iota(jnp.int32, old.shape, 1)
    want = tgt_ref[...] - step * width
    for i, col in enumerate(cols):
        total = total + jnp.exp(col - top)
        pick = jnp.where(want - i * lanes == lane, col, pick)
    top_ref[...] = top
    sum_ref[...] = total
    pick_ref[...] = pick


def head_stats(hid, w_head, tgt_loc):
    rows, d_model = hid.shape
    vocab_loc = w_head.shape[1]
    tile, lanes = 1024, 128
    lane_block = pl.BlockSpec((rows, lanes), lambda i: (0, 0))
    top, total, pick = pl.pallas_call(
        head_kernel,
        grid=(vocab_loc // tile,),
        in_specs=[
            pl.BlockSpec((rows, d_model), lambda i: (0, 0)),
            pl.BlockSpec((d_model, tile), lambda i: (0, i)),
            pl.BlockSpec((rows, 1), lambda i: (0, 0)),
        ],
        out_specs=[lane_block] * 3,
        out_shape=[jax.ShapeDtypeStruct((rows, lanes), F32)] * 3,
        cost_estimate=pl.CostEstimate(flops=2 * rows * d_model * vocab_loc, bytes_accessed=2 * d_model * vocab_loc,
                                      transcendentals=rows * vocab_loc),
    )(hid, w_head, tgt_loc[:, None])
    top_row = jnp.max(top, axis=1)
    sum_row = jnp.sum(total * jnp.exp(top - top_row[:, None]), axis=1)
    return top_row, sum_row, jnp.sum(pick, axis=1)


def hop(val, axis, pairs):
    return lax.ppermute(val, axis, pairs)


def gather_resp(val):
    return jnp.concatenate([val] + [hop(val, 'resp', [(i, i ^ b) for i in range(4)]) for b in (1, 2, 3)], axis=0)


RIGHT = [(0, 1), (1, 2), (2, 3)]
LEFT = [(1, 0), (2, 1), (3, 2)]


ORDER = (
    'Q00', 'W00', 'Q10', 'V00', 'O00', 'O10', 'G00', 'Q20', 'G10', 'I00', 'O20', 'I10',
    'M00', 'W01', 'M10', 'V01', 'S00', 'G20', 'S10', 'I20', 'T00', 'M20', 'T10', 'X00',
    'S20', 'X10', 'H00', 'J00', 'T20', 'H10', 'Q01', 'X20', 'J10', 'O01', 'H20', 'Q11',
    'G01', 'J20', 'O11', 'Q21', 'I01', 'G11', 'M01', 'I11', 'O21', 'S01', 'M11', 'T01',
    'G21', 'S11', 'I21', 'X01', 'M21', 'T11', 'H01', 'S21', 'J01', 'X11', 'L01', 'H11',
    'T21', 'J11', 'X21', 'L11', 'H21', 'J21', 'L21',
)


def solution(mesh):
    group_size = mesh.shape['resp']
    rows_spec = P(('prompts', 'resp'), None)
    in_specs = (rows_spec, P(('prompts', 'resp'), None, None), rows_spec, P(), P(),
                P(None, None, 'model', None), P(None, None, 'model', None), P(None, None, 'model', None),
                P(None, 'model', None, None), P(None, None, 'model'), P(None, None, 'model'),
                P(None, 'model', None), P(), P(None, 'model'))

    def local_pass(x_piece, x_own, tgt_own, attn_norm, mlp_norm, w_q, w_k, w_v, w_o, w_gate, w_up, w_down, final_norm, w_head):
        piece_len, d_model = x_piece.shape
        resp_len = x_own.shape[1]
        head_dim = w_q.shape[3]
        prompt_len = piece_len * group_size
        dev_idx = lax.axis_index('resp')
        model_idx = lax.axis_index('model')
        plane_idx = lax.axis_index('prompts') * group_size + dev_idx
        edges = [resp_len * s // 16 for s in SPLITS]
        n_chunks = len(edges) - 1

        def block_of(rows, owner):
            blk = rows.shape[0] // 4
            return lax.dynamic_slice_in_dim(rows, owner * blk, blk, 0)

        n_rep = mesh.shape['prompts'] * group_size
        w_o_flat = w_o.reshape(w_o.shape[0], -1, d_model)
        part = w_o_flat.shape[1] // n_rep

        w_o_mine = [lax.dynamic_slice_in_dim(w_o_flat[i], plane_idx * part, part, 0) for i in range(2)]
        w_o_sent = [None, None]
        w_o_all = [None, None]

        resp_pos = prompt_len + jnp.arange(resp_len)
        pos = [resp_pos[lo:hi] for lo, hi in zip(edges[:-1], edges[1:])]
        x_full = [x_own[0, lo:hi] for lo, hi in zip(edges[:-1], edges[1:])]
        tgt = [tgt_own[0, lo:hi] for lo, hi in zip(edges[:-1], edges[1:])]
        pos[0] = jnp.concatenate([dev_idx * piece_len + jnp.arange(piece_len), pos[0]])
        x_full[0] = jnp.concatenate([x_piece, x_full[0]], axis=0)
        rope = [rope_tables(p, head_dim) for p in pos]
        prompt_k_pos = jnp.concatenate([(dev_idx ^ b) * piece_len + jnp.arange(piece_len) for b in range(4)])

        w_q_flat = w_q.reshape(w_q.shape[0], d_model, -1)
        w_k_flat = w_k.reshape(w_k.shape[0], d_model, -1)
        w_v_flat = w_v.reshape(w_v.shape[0], d_model, -1)

        def kv_proj(hidden, layer, tabs):
            k_tok = rope_flat(jnp.dot(hidden, w_k_flat[layer], preferred_element_type=F32), *tabs)
            v_tok = jnp.dot(hidden, w_v_flat[layer], preferred_element_type=F32)
            return jnp.concatenate([k_tok, v_tok], axis=1).astype(BF16)

        x_blk = [block_of(x, model_idx) for x in x_full]
        state = [dict() for _ in range(n_chunks)]
        kv_prompt = [None, None]
        kv_own = [[], []]
        stats = [None] * n_chunks
        token = []

        def after(*vals):
            flat = lax.optimization_barrier(tuple(vals) + tuple(token))
            return list(flat[:len(vals)])

        def run_send(c, layer):
            mine, = after(w_o_mine[layer])
            w_o_sent[layer] = [hop(mine, 'model', [(i, (i - d) % 4) for i in range(4)]) for d in (1, 2, 3)]
            return [mine]

        def run_gather(c, layer):
            sent = after(*w_o_sent[layer])
            w_o_all[layer] = [w_o_flat[layer]] + [lax.all_gather(s, ('prompts', 'resp'), axis=0, tiled=True) for s in sent]
            return sent

        def spread(c, rows):
            st = state[c]
            st['own'] = rows
            st['l1'] = hop(rows, 'model', RIGHT)
            st['r1'] = hop(rows, 'model', LEFT)
            return [rows]

        def forward(c, layer):
            st = state[c]
            st['l1'], st['r1'] = after(st['l1'], st['r1'])
            st['l2'] = hop(st['l1'], 'model', [(1, 2), (2, 3)])
            st['r2'] = hop(st['r1'], 'model', [(2, 1), (1, 0)])
            return [st['l1'], st['r1']]

        def forward_last(c, layer):
            st = state[c]
            st['l2'], st['r2'] = after(st['l2'], st['r2'])
            st['mid'] = st['l2'] + st['r2']
            st['end'] = hop(st['mid'], 'model', [(2, 3), (1, 0)])
            return [st['mid']]

        def collect(c):
            own, l1, r1, mid, end = after(*[state[c][k] for k in ('own', 'l1', 'r1', 'mid', 'end')])
            blocks = []
            for b in range(4):
                away = model_idx - b
                val = jnp.where(away == 0, own, jnp.where(away == 1, l1, jnp.where(away == -1, r1, jnp.where(abs(away) == 2, mid, end))))
                blocks.append(val)
            return jnp.concatenate(blocks, axis=0)

        def run_attn(c, layer):
            x_all, = after(x_full[c]) if layer == 0 else [collect(c)]
            hid = rms_norm(x_all, attn_norm[layer])
            kv = kv_proj(hid, layer, rope[c])
            tabs, q_pos = rope[c], pos[c]
            mixes = []
            if c == 0:
                kv_prompt[layer] = gather_resp(kv[:piece_len])
                kv_own[layer].append(kv[piece_len:])
                if layer == 1:
                    hid, x_all = hid[piece_len:], x_all[piece_len:]
                    x_blk[0] = block_of(x_all, model_idx)
                q_f = jnp.dot(hid, w_q_flat[layer], preferred_element_type=F32)
                if layer == 0:
                    mixes.append(attend(q_f[:piece_len], tabs[0][:piece_len], tabs[1][:piece_len], kv_prompt[0],
                                        q_pos[:piece_len], prompt_k_pos, 0, head_dim))
                    q_f = q_f[piece_len:]
                tabs, q_pos = [t[piece_len:] for t in tabs], q_pos[piece_len:]
                kv_rows = jnp.concatenate([kv_prompt[layer]] + kv_own[layer], axis=0)
            else:
                q_f = jnp.dot(hid, w_q_flat[layer], preferred_element_type=F32)
                kv_own[layer].append(kv)
                kv_rows = jnp.concatenate([kv_prompt[layer]] + kv_own[layer], axis=0)
            mixes.append(attend(q_f, *tabs, kv_rows, q_pos, q_pos, kv_rows.shape[0] - q_pos.shape[0], head_dim))
            mix = jnp.concatenate(mixes, axis=0)
            state[c]['mix'] = [block_of(mix, model_idx)]
            for d in (1, 2, 3):
                rows = block_of(mix, (model_idx + 4 - d) % 4)
                state[c]['mix'].append(hop(rows, 'model', [(i, (i - d) % 4) for i in range(4)]))
            return [mix]

        def run_out(c, layer):
            total = None
            for rows, w_part in zip(after(*state[c]['mix']), w_o_all[layer]):
                term = jnp.dot(rows, w_part, preferred_element_type=F32)
                total = term if total is None else total + term
            x_blk[c] = (x_blk[c].astype(F32) + total).astype(BF16)
            return spread(c, rms_norm(x_blk[c], mlp_norm[layer]))

        def run_mlp(c, layer):
            hidden = collect(c)
            gate_proj = jnp.dot(hidden, w_gate[layer], preferred_element_type=F32)
            up_proj = jnp.dot(hidden, w_up[layer], preferred_element_type=F32)
            act = (jax.nn.silu(gate_proj) * up_proj).astype(BF16)
            part = jnp.dot(act, w_down[layer], preferred_element_type=F32)
            st = state[c]
            st['part'] = [block_of(part, (model_idx + 4 - d) % 4) for d in range(4)]
            st['far'] = hop(block_of(part, jnp.where(model_idx == 0, 3, 0)), 'model', [(0, 1), (3, 2)])
            return [part]

        def run_sum(c, layer):
            st = state[c]
            far, two = after(st['far'], st['part'][2])
            two = two + far
            st['right'] = hop(two, 'model', [(0, 1), (1, 2)])
            st['left'] = hop(two, 'model', [(3, 2), (2, 1)])
            return [two]

        def run_last(c, layer):
            st = state[c]
            right, left, p3, p1 = after(st['right'], st['left'], st['part'][3], st['part'][1])
            to_right, to_left = p3 + right, p1 + left
            st['right'] = hop(to_right, 'model', RIGHT)
            st['left'] = hop(to_left, 'model', LEFT)
            return [to_right, to_left]

        def run_next(c, layer):
            right, left, own = after(state[c]['right'], state[c]['left'], state[c]['part'][0])
            x_blk[c] = (x_blk[c].astype(F32) + (own + right + left)).astype(BF16)
            return spread(c, rms_norm(x_blk[c], final_norm) if layer == 1 else x_blk[c])

        vocab_loc = w_head.shape[1]

        def run_head(c, layer):
            stats[c] = jnp.stack(head_stats(collect(c), w_head, tgt[c] - model_idx * vocab_loc))
            return [stats[c]]

        run = {'Q': run_attn, 'O': run_out, 'M': run_mlp, 'S': run_sum, 'T': run_last, 'W': run_send, 'V': run_gather, 'X': run_next, 'L': run_head,
               'G': forward, 'I': forward_last, 'H': forward, 'J': forward_last}
        for step in ORDER:
            token = run[step[0]](int(step[1]), int(step[2]))

        every = lax.all_gather(jnp.concatenate(stats, axis=1), 'model')
        top_all = jnp.max(every[:, 0], axis=0)
        exp_all = jnp.sum(every[:, 1] * jnp.exp(every[:, 0] - top_all[None]), axis=0)
        picked_all = jnp.sum(every[:, 2], axis=0)
        return (picked_all - top_all - jnp.log(exp_all))[None, :]

    return jax.shard_map(local_pass, mesh=mesh, in_specs=in_specs, out_specs=rows_spec, check_vma=False)
```

```python
import math
import jax
import jax.numpy as jnp
from jax import lax
from jax.experimental import pallas as pl
from jax.experimental.pallas import tpu as pltpu
from jax.sharding import PartitionSpec as P

RMS_EPS = 1e-6
ROPE_BASE = 10000.0
NEG_BIG = -1e30
SPLITS = (0, 4, 10, 16)


F32 = jnp.float32
BF16 = jnp.bfloat16


def rms_norm(x_in, norm_gain):
    x_f = x_in.astype(F32)
    mean_sq = jnp.mean(x_f * x_f, axis=-1, keepdims=True)
    return (x_f * lax.rsqrt(mean_sq + RMS_EPS) * norm_gain).astype(BF16)


def rope_tables(positions, head_dim):
    inv_freq = jnp.exp(jnp.arange(0, head_dim, 2, dtype=F32) * (-math.log(ROPE_BASE) / head_dim))
    angles = positions.astype(F32)[:, None] * inv_freq[None, :]
    cos_t, sin_t = jnp.cos(angles), jnp.sin(angles)
    return jnp.concatenate([cos_t, cos_t], axis=1), jnp.concatenate([-sin_t, sin_t], axis=1)


def rope_flat(proj_f, cos_tab, sin_tab):
    head_dim = cos_tab.shape[1]
    half_dim = head_dim // 2
    out = []
    for h in range(proj_f.shape[1] // head_dim):
        lo_half = proj_f[:, h * head_dim:h * head_dim + half_dim]
        hi_half = proj_f[:, h * head_dim + half_dim:(h + 1) * head_dim]
        out.append(lo_half * cos_tab[:, :half_dim] - hi_half * sin_tab[:, half_dim:])
        out.append(hi_half * cos_tab[:, half_dim:] + lo_half * sin_tab[:, half_dim:])
    return jnp.concatenate(out, axis=1)


def attn_kernel(n_free, q_ref, cos_ref, sin_ref, k_ref, v_ref, q_pos_ref, k_pos_ref, out_ref):
    head_dim = k_ref.shape[1]
    scale = 1.0 / math.sqrt(head_dim)
    cos_t, sin_t = cos_ref[...], sin_ref[...]
    seen = k_pos_ref[...] <= q_pos_ref[...]
    contract = (((1,), (1,)), ((), ()))
    for h in range(q_ref.shape[1] // head_dim):
        cols = slice(h * head_dim, (h + 1) * head_dim)
        q_f = q_ref[:, cols]
        q_b = (q_f * cos_t + pltpu.roll(q_f, head_dim // 2, 1) * sin_t).astype(BF16)
        s_own = lax.dot_general(q_b, k_ref[n_free:], contract, preferred_element_type=F32) * scale
        s_own = jnp.where(seen, s_own, NEG_BIG)
        top = jnp.max(s_own, axis=1, keepdims=True)
        if n_free:
            s_free = lax.dot_general(q_b, k_ref[:n_free], contract, preferred_element_type=F32) * scale
            top = jnp.maximum(top, jnp.max(s_free, axis=1, keepdims=True))
            e_free = jnp.exp(s_free - top)
        e_own = jnp.exp(s_own - top)
        total = jnp.sum(e_own, axis=1, keepdims=True)
        if n_free:
            total = total + jnp.sum(e_free, axis=1, keepdims=True)
        inv = 1.0 / total
        mix = jnp.dot((e_own * inv).astype(BF16), v_ref[n_free:], preferred_element_type=F32)
        if n_free:
            mix = mix + jnp.dot((e_free * inv).astype(BF16), v_ref[:n_free], preferred_element_type=F32)
        out_ref[:, cols] = mix.astype(BF16)


def attend(q_f, cos_tab, sin_tab, kv_rows, q_pos, k_pos, n_free, head_dim):
    rows, width = q_f.shape
    n_keys = kv_rows.shape[0]
    n_kv = kv_rows.shape[1] // (2 * head_dim)
    grp = width // n_kv
    tile = 128
    return pl.pallas_call(
        lambda *refs: attn_kernel(n_free, *refs),
        grid=(n_kv, rows // tile),
        in_specs=[
            pl.BlockSpec((tile, grp), lambda g, i: (i, g)),
            pl.BlockSpec((tile, head_dim), lambda g, i: (i, 0)),
            pl.BlockSpec((tile, head_dim), lambda g, i: (i, 0)),
            pl.BlockSpec((n_keys, head_dim), lambda g, i: (0, g)),
            pl.BlockSpec((n_keys, head_dim), lambda g, i: (0, n_kv + g)),
            pl.BlockSpec((tile, 1), lambda g, i: (i, 0)),
            pl.BlockSpec((1, n_keys - n_free), lambda g, i: (0, 0)),
        ],
        out_specs=pl.BlockSpec((tile, grp), lambda g, i: (i, g)),
        out_shape=jax.ShapeDtypeStruct((rows, width), BF16),
        cost_estimate=pl.CostEstimate(flops=4 * rows * n_keys * width, bytes_accessed=6 * rows * width + 2 * n_keys * kv_rows.shape[1],
                                      transcendentals=rows * n_keys * (width // head_dim)),
    )(q_f, cos_tab, sin_tab, kv_rows, kv_rows, q_pos[:, None], k_pos[None, :])


def head_kernel(hid_ref, w_ref, tgt_ref, top_ref, sum_ref, pick_ref):
    step = pl.program_id(0)
    lanes = top_ref.shape[1]
    width = w_ref.shape[1]

    @pl.when(step == 0)
    def _():
        top_ref[...] = jnp.full_like(top_ref, NEG_BIG)
        sum_ref[...] = jnp.zeros_like(sum_ref)
        pick_ref[...] = jnp.zeros_like(pick_ref)

    logits = jnp.dot(hid_ref[...], w_ref[...], preferred_element_type=F32)
    cols = [logits[:, i * lanes:(i + 1) * lanes] for i in range(width // lanes)]
    old = top_ref[...]
    top = old
    for col in cols:
        top = jnp.maximum(top, col)
    total = sum_ref[...] * jnp.exp(old - top)
    pick = pick_ref[...]
    lane = lax.broadcasted_iota(jnp.int32, old.shape, 1)
    want = tgt_ref[...] - step * width
    for i, col in enumerate(cols):
        total = total + jnp.exp(col - top)
        pick = jnp.where(want - i * lanes == lane, col, pick)
    top_ref[...] = top
    sum_ref[...] = total
    pick_ref[...] = pick


def head_stats(hid, w_head, tgt_loc):
    rows, d_model = hid.shape
    vocab_loc = w_head.shape[1]
    tile, lanes = 1024, 128
    lane_block = pl.BlockSpec((rows, lanes), lambda i: (0, 0))
    top, total, pick = pl.pallas_call(
        head_kernel,
        grid=(vocab_loc // tile,),
        in_specs=[
            pl.BlockSpec((rows, d_model), lambda i: (0, 0)),
            pl.BlockSpec((d_model, tile), lambda i: (0, i)),
            pl.BlockSpec((rows, 1), lambda i: (0, 0)),
        ],
        out_specs=[lane_block] * 3,
        out_shape=[jax.ShapeDtypeStruct((rows, lanes), F32)] * 3,
        cost_estimate=pl.CostEstimate(flops=2 * rows * d_model * vocab_loc, bytes_accessed=2 * d_model * vocab_loc,
                                      transcendentals=rows * vocab_loc),
    )(hid, w_head, tgt_loc[:, None])
    top_row = jnp.max(top, axis=1)
    sum_row = jnp.sum(total * jnp.exp(top - top_row[:, None]), axis=1)
    return top_row, sum_row, jnp.sum(pick, axis=1)


def hop(val, axis, pairs):
    return lax.ppermute(val, axis, pairs)


def gather_resp(val):
    return jnp.concatenate([val] + [hop(val, 'resp', [(i, i ^ b) for i in range(4)]) for b in (1, 2, 3)], axis=0)


RIGHT = [(0, 1), (1, 2), (2, 3)]
LEFT = [(1, 0), (2, 1), (3, 2)]


ORDER = (
    'Q00', 'W00', 'Q10', 'V00', 'Q20', 'O00', 'O10', 'G00', 'G10', 'I00', 'O20', 'I10',
    'M00', 'W01', 'M10', 'V01', 'S00', 'G20', 'S10', 'I20', 'T00', 'M20', 'T10', 'X00',
    'S20', 'X10', 'H00', 'J00', 'T20', 'H10', 'Q01', 'X20', 'J10', 'O01', 'H20', 'Q11',
    'G01', 'J20', 'O11', 'Q21', 'I01', 'G11', 'M01', 'I11', 'O21', 'S01', 'M11', 'T01',
    'G21', 'S11', 'I21', 'X01', 'M21', 'T11', 'H01', 'S21', 'J01', 'X11', 'L01', 'H11',
    'T21', 'J11', 'X21', 'L11', 'H21', 'J21', 'L21',
)


def solution(mesh):
    group_size = mesh.shape['resp']
    rows_spec = P(('prompts', 'resp'), None)
    in_specs = (rows_spec, P(('prompts', 'resp'), None, None), rows_spec, P(), P(),
                P(None, None, 'model', None), P(None, None, 'model', None), P(None, None, 'model', None),
                P(None, 'model', None, None), P(None, None, 'model'), P(None, None, 'model'),
                P(None, 'model', None), P(), P(None, 'model'))

    def local_pass(x_piece, x_own, tgt_own, attn_norm, mlp_norm, w_q, w_k, w_v, w_o, w_gate, w_up, w_down, final_norm, w_head):
        piece_len, d_model = x_piece.shape
        resp_len = x_own.shape[1]
        head_dim = w_q.shape[3]
        prompt_len = piece_len * group_size
        dev_idx = lax.axis_index('resp')
        model_idx = lax.axis_index('model')
        plane_idx = lax.axis_index('prompts') * group_size + dev_idx
        edges = [resp_len * s // 16 for s in SPLITS]
        n_chunks = len(edges) - 1

        def block_of(rows, owner):
            blk = rows.shape[0] // 4
            return lax.dynamic_slice_in_dim(rows, owner * blk, blk, 0)

        n_rep = mesh.shape['prompts'] * group_size
        w_o_flat = w_o.reshape(w_o.shape[0], -1, d_model)
        part = w_o_flat.shape[1] // n_rep

        w_o_mine = [lax.dynamic_slice_in_dim(w_o_flat[i], plane_idx * part, part, 0) for i in range(2)]
        w_o_sent = [None, None]
        w_o_all = [None, None]

        resp_pos = prompt_len + jnp.arange(resp_len)
        pos = [resp_pos[lo:hi] for lo, hi in zip(edges[:-1], edges[1:])]
        x_full = [x_own[0, lo:hi] for lo, hi in zip(edges[:-1], edges[1:])]
        tgt = [tgt_own[0, lo:hi] for lo, hi in zip(edges[:-1], edges[1:])]
        pos[0] = jnp.concatenate([dev_idx * piece_len + jnp.arange(piece_len), pos[0]])
        x_full[0] = jnp.concatenate([x_piece, x_full[0]], axis=0)
        rope = [rope_tables(p, head_dim) for p in pos]
        prompt_k_pos = jnp.concatenate([(dev_idx ^ b) * piece_len + jnp.arange(piece_len) for b in range(4)])

        w_q_flat = w_q.reshape(w_q.shape[0], d_model, -1)
        w_k_flat = w_k.reshape(w_k.shape[0], d_model, -1)
        w_v_flat = w_v.reshape(w_v.shape[0], d_model, -1)

        def kv_proj(hidden, layer, tabs):
            k_tok = rope_flat(jnp.dot(hidden, w_k_flat[layer], preferred_element_type=F32), *tabs)
            v_tok = jnp.dot(hidden, w_v_flat[layer], preferred_element_type=F32)
            return jnp.concatenate([k_tok, v_tok], axis=1).astype(BF16)

        x_blk = [block_of(x, model_idx) for x in x_full]
        state = [dict() for _ in range(n_chunks)]
        kv_prompt = [None, None]
        kv_own = [[], []]
        stats = [None] * n_chunks
        token = []

        def after(*vals):
            flat = lax.optimization_barrier(tuple(vals) + tuple(token))
            return list(flat[:len(vals)])

        def run_send(c, layer):
            mine, = after(w_o_mine[layer])
            w_o_sent[layer] = [hop(mine, 'model', [(i, (i - d) % 4) for i in range(4)]) for d in (1, 2, 3)]
            return [mine]

        def run_gather(c, layer):
            sent = after(*w_o_sent[layer])
            w_o_all[layer] = [w_o_flat[layer]] + [lax.all_gather(s, ('prompts', 'resp'), axis=0, tiled=True) for s in sent]
            return sent

        def spread(c, rows):
            st = state[c]
            st['own'] = rows
            st['l1'] = hop(rows, 'model', RIGHT)
            st['r1'] = hop(rows, 'model', LEFT)
            return [rows]

        def forward(c, layer):
            st = state[c]
            st['l1'], st['r1'] = after(st['l1'], st['r1'])
            st['l2'] = hop(st['l1'], 'model', [(1, 2), (2, 3)])
            st['r2'] = hop(st['r1'], 'model', [(2, 1), (1, 0)])
            return [st['l1'], st['r1']]

        def forward_last(c, layer):
            st = state[c]
            st['l2'], st['r2'] = after(st['l2'], st['r2'])
            st['mid'] = st['l2'] + st['r2']
            st['end'] = hop(st['mid'], 'model', [(2, 3), (1, 0)])
            return [st['mid']]

        def collect(c):
            own, l1, r1, mid, end = after(*[state[c][k] for k in ('own', 'l1', 'r1', 'mid', 'end')])
            blocks = []
            for b in range(4):
                away = model_idx - b
                val = jnp.where(away == 0, own, jnp.where(away == 1, l1, jnp.where(away == -1, r1, jnp.where(abs(away) == 2, mid, end))))
                blocks.append(val)
            return jnp.concatenate(blocks, axis=0)

        def run_attn(c, layer):
            x_all, = after(x_full[c]) if layer == 0 else [collect(c)]
            hid = rms_norm(x_all, attn_norm[layer])
            kv = kv_proj(hid, layer, rope[c])
            tabs, q_pos = rope[c], pos[c]
            mixes = []
            if c == 0:
                kv_prompt[layer] = gather_resp(kv[:piece_len])
                kv_own[layer].append(kv[piece_len:])
                if layer == 1:
                    hid, x_all = hid[piece_len:], x_all[piece_len:]
                    x_blk[0] = block_of(x_all, model_idx)
                q_f = jnp.dot(hid, w_q_flat[layer], preferred_element_type=F32)
                if layer == 0:
                    mixes.append(attend(q_f[:piece_len], tabs[0][:piece_len], tabs[1][:piece_len], kv_prompt[0],
                                        q_pos[:piece_len], prompt_k_pos, 0, head_dim))
                    q_f = q_f[piece_len:]
                tabs, q_pos = [t[piece_len:] for t in tabs], q_pos[piece_len:]
                kv_rows = jnp.concatenate([kv_prompt[layer]] + kv_own[layer], axis=0)
            else:
                q_f = jnp.dot(hid, w_q_flat[layer], preferred_element_type=F32)
                kv_own[layer].append(kv)
                kv_rows = jnp.concatenate([kv_prompt[layer]] + kv_own[layer], axis=0)
            mixes.append(attend(q_f, *tabs, kv_rows, q_pos, q_pos, kv_rows.shape[0] - q_pos.shape[0], head_dim))
            mix = jnp.concatenate(mixes, axis=0)
            state[c]['mix'] = [block_of(mix, model_idx)]
            for d in (1, 2, 3):
                rows = block_of(mix, (model_idx + 4 - d) % 4)
                state[c]['mix'].append(hop(rows, 'model', [(i, (i - d) % 4) for i in range(4)]))
            return [mix]

        def run_out(c, layer):
            total = None
            for rows, w_part in zip(after(*state[c]['mix']), w_o_all[layer]):
                term = jnp.dot(rows, w_part, preferred_element_type=F32)
                total = term if total is None else total + term
            x_blk[c] = (x_blk[c].astype(F32) + total).astype(BF16)
            return spread(c, rms_norm(x_blk[c], mlp_norm[layer]))

        def run_mlp(c, layer):
            hidden = collect(c)
            gate_proj = jnp.dot(hidden, w_gate[layer], preferred_element_type=F32)
            up_proj = jnp.dot(hidden, w_up[layer], preferred_element_type=F32)
            act = (jax.nn.silu(gate_proj) * up_proj).astype(BF16)
            part = jnp.dot(act, w_down[layer], preferred_element_type=F32)
            st = state[c]
            st['part'] = [block_of(part, (model_idx + 4 - d) % 4) for d in range(4)]
            st['far'] = hop(block_of(part, jnp.where(model_idx == 0, 3, 0)), 'model', [(0, 1), (3, 2)])
            return [part]

        def run_sum(c, layer):
            st = state[c]
            far, two = after(st['far'], st['part'][2])
            two = two + far
            st['right'] = hop(two, 'model', [(0, 1), (1, 2)])
            st['left'] = hop(two, 'model', [(3, 2), (2, 1)])
            return [two]

        def run_last(c, layer):
            st = state[c]
            right, left, p3, p1 = after(st['right'], st['left'], st['part'][3], st['part'][1])
            to_right, to_left = p3 + right, p1 + left
            st['right'] = hop(to_right, 'model', RIGHT)
            st['left'] = hop(to_left, 'model', LEFT)
            return [to_right, to_left]

        def run_next(c, layer):
            right, left, own = after(state[c]['right'], state[c]['left'], state[c]['part'][0])
            x_blk[c] = (x_blk[c].astype(F32) + (own + right + left)).astype(BF16)
            return spread(c, rms_norm(x_blk[c], final_norm) if layer == 1 else x_blk[c])

        vocab_loc = w_head.shape[1]

        def run_head(c, layer):
            stats[c] = jnp.stack(head_stats(collect(c), w_head, tgt[c] - model_idx * vocab_loc))
            return [stats[c]]

        run = {'Q': run_attn, 'O': run_out, 'M': run_mlp, 'S': run_sum, 'T': run_last, 'W': run_send, 'V': run_gather, 'X': run_next, 'L': run_head,
               'G': forward, 'I': forward_last, 'H': forward, 'J': forward_last}
        for step in ORDER:
            token = run[step[0]](int(step[1]), int(step[2]))

        every = lax.all_gather(jnp.concatenate(stats, axis=1), 'model')
        top_all = jnp.max(every[:, 0], axis=0)
        exp_all = jnp.sum(every[:, 1] * jnp.exp(every[:, 0] - top_all[None]), axis=0)
        picked_all = jnp.sum(every[:, 2], axis=0)
        return (picked_all - top_all - jnp.log(exp_all))[None, :]

    return jax.shard_map(local_pass, mesh=mesh, in_specs=in_specs, out_specs=rows_spec, check_vma=False)
```
